16 devices in a mesh: row: 2 (over z), col: 8 (over y, x, core).
Axes of the slice: x: 2, y: 2, z: 2, core: 2. Of those that a mesh axis runs over, the one named last changes fastest.
Arguments:
- v_panels: float32 [8192, 8192], P('row', 'col')
- t_factors: float32 [64, 128, 128], P('col')
- z_vectors: float32 [8192, 4096], P(None, ('col', 'row'))
Outputs:
- output: float32 [8192, 4096], P('row', 'col')
All inputs are finite; a program needn't handle non-finite values.
Results may differ from the reference program's by a relative error of at most 0.001.
Values sent between devices are 32-bit elements.
A program may use at most 1 GiB of HBM per device.

```python
import jax
import jax.numpy as jnp
from jax import lax

N = 8192
B = 128
K = 4096


def build_factors(v_panels):
    panel_count = N // B
    v_blocks = v_panels.reshape(N, panel_count, B).astype(jnp.float32)
    gram_mat = jnp.einsum("nmp,nmq->mpq", v_blocks, v_blocks)
    tau_all = 2.0 / jnp.diagonal(gram_mat, axis1=1, axis2=2)
    lane_ids = jnp.arange(B)

    def add_column(col_idx, t_acc):
        g_col = lax.dynamic_index_in_dim(gram_mat, col_idx, axis=2, keepdims=False)
        g_col = jnp.where(lane_ids[None, :] < col_idx, g_col, 0.0)
        tau_col = lax.dynamic_index_in_dim(tau_all, col_idx, axis=1, keepdims=True)
        new_col = -tau_col * jnp.einsum("mpq,mq->mp", t_acc, g_col)
        new_col = jnp.where(lane_ids[None, :] == col_idx, tau_col, new_col)
        return jnp.where(lane_ids[None, None, :] == col_idx, new_col[:, :, None], t_acc)

    t_start = jnp.zeros((panel_count, B, B), jnp.float32)
    return lax.fori_loop(0, B, add_column, t_start)


def setup_inputs(seed: int = 0) -> dict:
    key = jax.random.key(seed)
    key_v, key_z = jax.random.split(key)
    raw_v = jax.random.normal(key_v, (N, N), jnp.float32)
    row_ids = jnp.arange(N)[:, None]
    col_ids = jnp.arange(N)[None, :]
    in_block = (row_ids // B) == (col_ids // B)
    scaled = raw_v * jnp.where(in_block, B ** -0.5, 1.0)
    v_panels = jnp.where(row_ids > col_ids, scaled, jnp.where(row_ids == col_ids, 1.0, 0.0)).astype(jnp.float32)
    t_factors = build_factors(v_panels)
    z_vectors = jax.random.normal(key_z, (N, K), jnp.float32)
    return {"v_panels": v_panels, "t_factors": t_factors, "z_vectors": z_vectors}


def reference(v_panels, t_factors, z_vectors):
    panel_count = N // B

    def apply_panel(step, x_cur):
        panel_idx = panel_count - 1 - step
        v_pan = lax.dynamic_slice_in_dim(v_panels, panel_idx * B, B, axis=1)
        t_pan = lax.dynamic_index_in_dim(t_factors, panel_idx, axis=0, keepdims=False)
        w_mat = lax.dot_general(v_pan, x_cur, (((0,), (0,)), ((), ())), precision=lax.Precision.HIGHEST, preferred_element_type=jnp.float32)
        y_mat = jnp.dot(t_pan, w_mat, precision=lax.Precision.HIGHEST, preferred_element_type=jnp.float32)
        return x_cur - jnp.dot(v_pan, y_mat, precision=lax.Precision.HIGHEST, preferred_element_type=jnp.float32)

    return lax.fori_loop(0, panel_count, apply_panel, z_vectors)
```

```python
import functools
import os

import jax
import jax.numpy as jnp
from jax import lax
from jax.experimental import pallas as pl
from jax.experimental.pallas import tpu as pltpu
from jax.sharding import PartitionSpec as P

HI = lax.Precision.HIGHEST
MESH = pl.DeviceIdType.MESH
NCH = 32
NT = NCH * (NCH + 1) // 2
HOP = 6
PRE = 4
LATE = 4 * HOP + 3
LAG = LATE + PRE
RING = 32
LRING = 8


def dot(a, b):
    return jnp.dot(a, b, precision=HI, preferred_element_type=jnp.float32)


def dot_t(a, b):
    return lax.dot_general(a, b, (((0,), (0,)), ((), ())), precision=HI, preferred_element_type=jnp.float32)


def kernel(ts, v_ref, t_ref, z_ref, out_ref, vb_ref, tb_ref, xs, vv, ws, gs, ys, tv,
           recv, recv_t, snd, snd_t, lsem, tsem, zsem, osem, orecv):
    hb = ts // 2
    z = lax.axis_index("row")
    col = lax.axis_index("col")
    core = lax.rem(col, 2)
    x = lax.rem(col // 2, 2)
    y = col // 4
    half = NCH // 2

    def flip(q):
        nx = jnp.where(q == 0, 1 - x, x)
        ny = jnp.where(q == 1, 1 - y, y)
        nz = jnp.where(q == 2, 1 - z, z)
        return (nz, (ny * 2 + nx) * 2 + core)

    sibling = (z, col + 1 - 2 * core)
    neighbours = [flip(0), flip(1), flip(2), sibling]

    zcopy = pltpu.make_async_copy(z_ref, xs, zsem)
    zcopy.start()
    barrier = pltpu.get_barrier_semaphore()
    for d in neighbours:
        pl.semaphore_signal(barrier, inc=1, device_id=d, device_id_type=MESH)
    pl.semaphore_wait(barrier, 4)

    def role(n, i, t):
        g = NCH - 1 - i
        rho = g + t
        ro = rho // half
        co = g // 4
        ax = lax.rem(x + lax.rem(co // 2, 2), 2)
        ay = lax.rem(y + co // 4, 2)
        az = lax.rem(z + ro, 2)
        k = lax.rem(n, 3)
        a = jnp.where(k == 0, ax, jnp.where(k == 1, ay, az))
        b = jnp.where(k == 0, ay, jnp.where(k == 1, az, ax))
        c = jnp.where(k == 0, az, jnp.where(k == 1, ax, ay))
        s = a + b + c
        mine = lax.rem(co, 2) == core
        return k, a, b, c, s, mine

    def v_src(i, t):
        g = NCH - 1 - i
        rho = g + t
        return v_ref.at[pl.ds(pl.multiple_of(lax.rem(rho, half) * ts, ts), ts),
                        pl.ds(pl.multiple_of(lax.rem(g, 4) * ts, ts), ts)]

    def t_src(i):
        g = NCH - 1 - i
        return t_ref.at[pl.ds(lax.rem(g, 4) * 2, 2)]

    def ship(root, n, i, t, kind, dev):
        cv = pltpu.make_async_remote_copy(
            src_ref=v_src(i, t) if root else vb_ref.at[n], dst_ref=vb_ref.at[n],
            send_sem=snd.at[kind, lax.rem(n, RING)], recv_sem=recv.at[n], device_id=dev, device_id_type=MESH)
        ct = pltpu.make_async_remote_copy(
            src_ref=t_src(i) if root else tb_ref.at[i], dst_ref=tb_ref.at[i],
            send_sem=snd_t.at[kind, i], recv_sem=recv_t.at[i], device_id=dev, device_id_type=MESH)
        return cv, ct

    def start(root, n, i, t, kind, dev):
        cv, ct = ship(root, n, i, t, kind, dev)
        cv.start()

        @pl.when(t == 0)
        def _():
            ct.start()

    def arrived(n, i, t):
        cv, ct = ship(False, n, i, t, 0, sibling)
        cv.wait_recv()

        @pl.when(t == 0)
        def _():
            ct.wait_recv()

    def sent(n, i, t, kind):
        cv, ct = ship(False, n, i, t, kind, sibling)
        cv.wait_send()

        @pl.when(t == 0)
        def _():
            ct.wait_send()

    def slot(tau, st):
        st = list(st)
        for d in range(6):
            i, t = st[2 * d], st[2 * d + 1]
            n = tau - (d * HOP if d < 5 else LATE)
            live = jnp.logical_and(n >= 0, n < NT)
            k, a, b, c, s, mine = role(n, i, t)
            depth = jnp.where(a == 1, s, jnp.where(s == 0, 0, 2 + s))
            if d < 5:
                @pl.when(jnp.logical_and(live, jnp.logical_and(mine, depth == d)))
                def _():
                    root = d == 0
                    if not root:
                        arrived(n, i, t)
                    if d == 0:
                        start(root, n, i, t, 0, flip(k))
                    if d == 1:
                        start(root, n, i, t, 1, flip(lax.rem(k + 1, 3)))
                        start(root, n, i, t, 2, flip(lax.rem(k + 2, 3)))
                    if d == 2:
                        start(root, n, i, t, 0, flip(k))

                        @pl.when(b == 1)
                        def _():
                            start(root, n, i, t, 2, flip(lax.rem(k + 2, 3)))
                    if d == 3:
                        @pl.when(a == 1)
                        def _():
                            start(root, n, i, t, 0, flip(k))
                    start(root, n, i, t, 3, sibling)
            else:
                @pl.when(jnp.logical_and(live, jnp.logical_not(mine)))
                def _():
                    arrived(n, i, t)

                @pl.when(jnp.logical_and(live, mine))
                def _():
                    sent(n, i, t, 3)

                    @pl.when(jnp.logical_or(s == 0, jnp.logical_and(a == 1, s >= 2)))
                    def _():
                        sent(n, i, t, 0)

                    @pl.when(jnp.logical_and(a == 1, s == 1))
                    def _():
                        sent(n, i, t, 1)

                    @pl.when(jnp.logical_and(a == 1, c == 0))
                    def _():
                        sent(n, i, t, 2)
            end = t + 1 > i
            ni = jnp.where(n >= 0, jnp.where(end, i + 1, i), i)
            nt = jnp.where(n >= 0, jnp.where(end, 0, t + 1), t)
            st[2 * d], st[2 * d + 1] = ni, nt
        return tuple(st)

    def is_owner(i, t):
        g = NCH - 1 - i
        return jnp.logical_and(g // 4 == col, (g + t) // half == z)

    def load(i, t):
        n = i * (i + 1) // 2 + t
        dst = vv.at[lax.rem(i, 2), t]
        sem = lsem.at[lax.rem(n, LRING)]
        own = is_owner(i, t)

        @pl.when(own)
        def _():
            pltpu.make_async_copy(v_src(i, t), dst, sem).start()

        @pl.when(jnp.logical_not(own))
        def _():
            pltpu.make_async_copy(vb_ref.at[n], dst, sem).start()

    def loaded(i, t):
        n = i * (i + 1) // 2 + t
        pltpu.make_async_copy(vb_ref.at[n], vv.at[lax.rem(i, 2), t], lsem.at[lax.rem(n, LRING)]).wait()

    def load_t(i):
        own = is_owner(i, 0)
        sem = tsem.at[lax.rem(i, 2)]

        @pl.when(own)
        def _():
            pltpu.make_async_copy(t_src(i), tv.at[lax.rem(i, 2)], sem).start()

        @pl.when(jnp.logical_not(own))
        def _():
            pltpu.make_async_copy(tb_ref.at[i], tv.at[lax.rem(i, 2)], sem).start()

    def loaded_t(i):
        pltpu.make_async_copy(tb_ref.at[i], tv.at[lax.rem(i, 2)], tsem.at[lax.rem(i, 2)]).wait()

    def rows(rho):
        return pl.ds(pl.multiple_of(rho * ts, ts), ts)

    zero = jnp.int32(0)
    st = (zero,) * 12
    st = lax.fori_loop(0, LAG, slot, st)
    zcopy.wait()
    load(zero, zero)

    def chunk(i, st):
        g = NCH - 1 - i
        now = lax.rem(i, 2)
        old = 1 - now
        base = i * (i + 1) // 2
        ws[...] = jnp.zeros_like(ws)
        gs[...] = jnp.zeros_like(gs)
        load_t(i)

        def unit(t, st):
            st = slot(base + t + LAG, st)

            @pl.when(t + PRE <= i)
            def _():
                load(i, t + PRE)
            loaded(i, t)

            @pl.when(t >= 1)
            def _():
                xs[rows(g + t), :] = xs[rows(g + t), :] - dot(vv[old, t - 1], ys[...])
            vt = vv[now, t]
            ws[...] += dot_t(vt, xs[rows(g + t), :])
            gs[...] += dot_t(vt[:, :hb], vt[:, hb:])
            return st

        st = lax.fori_loop(0, i + 1, unit, st)
        for p in range(PRE):
            @pl.when(jnp.logical_and(i + 1 < NCH, p <= i + 1))
            def _():
                load(i + 1, jnp.int32(p))
        loaded_t(i)
        y2 = dot(tv[now, 1], ws[hb:, :])
        ys[hb:, :] = y2
        ys[:hb, :] = dot(tv[now, 0], ws[:hb, :] - dot(gs[...], y2))
        return st

    lax.fori_loop(0, NCH, chunk, st)

    other = (1 - z, col)

    def place(rho):
        return out_ref.at[rows(lax.rem(rho, half)), pl.ds(pl.multiple_of(z * ts, ts), ts)]

    def away(q):
        rho = half * (1 - z) + q
        return pltpu.make_async_remote_copy(
            src_ref=xs.at[rows(rho), :], dst_ref=place(rho), send_sem=osem.at[q], recv_sem=orecv.at[q],
            device_id=other, device_id_type=MESH)

    def home(q):
        rho = half * z + q
        return pltpu.make_async_copy(xs.at[rows(rho), :], place(rho), osem.at[half + q])

    def last(send, first, q, carry):
        rho = first + q
        xs[rows(rho), :] = xs[rows(rho), :] - dot(vv[(NCH - 1) % 2, rho], ys[...])
        send(q).start()
        return carry

    lax.fori_loop(0, half, functools.partial(last, away, half * (1 - z)), 0)
    lax.fori_loop(0, half, functools.partial(last, home, half * z), 0)

    def drain(q, carry):
        home(q).wait()
        away(q).wait_send()
        away(q).wait_recv()
        return carry

    lax.fori_loop(0, half, drain, 0)


def solution(mesh):
    def local_program(v_local, t_local, z_local):
        n = z_local.shape[0]
        ts = n // NCH
        f32 = jnp.float32
        any_ = pl.BlockSpec(memory_space=pl.ANY)
        dma = pltpu.SemaphoreType.DMA
        out, _, _ = pl.pallas_call(
            functools.partial(kernel, ts),
            out_shape=(jax.ShapeDtypeStruct((n // 2, 2 * ts), f32),
                       jax.ShapeDtypeStruct((NT, ts, ts), f32),
                       jax.ShapeDtypeStruct((NCH, 2, ts // 2, ts // 2), f32)),
            in_specs=[any_] * 3,
            out_specs=(any_,) * 3,
            scratch_shapes=[
                pltpu.VMEM((n, ts), f32),
                pltpu.VMEM((2, NCH, ts, ts), f32),
                pltpu.VMEM((ts, ts), f32),
                pltpu.VMEM((ts // 2, ts // 2), f32),
                pltpu.VMEM((ts, ts), f32),
                pltpu.VMEM((2, 2, ts // 2, ts // 2), f32),
                dma((NT,)), dma((NCH,)), dma((4, RING)), dma((4, NCH)),
                dma((LRING,)), dma((2,)), dma, dma((NCH,)), dma((NCH // 2,)),
            ],
            compiler_params=pltpu.CompilerParams(collective_id=0, has_side_effects=True, vmem_limit_bytes=60 * 1024 * 1024),
            name="back_transform",
        )(v_local, t_local, z_local)
        return out

    return jax.shard_map(local_program, mesh=mesh, in_specs=(P("row", "col"), P("col", None, None), P(None, ("col", "row"))),
                         out_specs=P("row", "col"), check_vma=False)
```

```python
import functools

import jax
import jax.numpy as jnp
from jax import lax
from jax.experimental import pallas as pl
from jax.experimental.pallas import tpu as pltpu
from jax.sharding import PartitionSpec as P

HI = lax.Precision.HIGHEST
MESH = pl.DeviceIdType.MESH
NCH = 32
NU = NCH // 2
NT = NU * (NU + 1)
HOP = 5
PRE = 2
LATE = 5 * HOP + 2
LAG = LATE + PRE
RING = 32
LRING = 4
FIRST = NCH - 2


def dot(a, b):
    return jnp.dot(a, b, precision=HI, preferred_element_type=jnp.float32)


def dot_t(a, b):
    return lax.dot_general(a, b, (((0,), (0,)), ((), ())), precision=HI, preferred_element_type=jnp.float32)


def unit_of(i, t):
    half = NU // 2
    top = (NCH - 1 - i) // 2
    inner = jnp.where(lax.rem(t, 2) == 0, top + t // 2, half + t // 2)
    return jnp.where(t < 2 * (half - top), inner, top + t)


def split(v):
    high = v.astype(jnp.bfloat16)
    rest = v - high.astype(jnp.float32)
    mid = rest.astype(jnp.bfloat16)
    low = (rest - mid.astype(jnp.float32)).astype(jnp.bfloat16)
    return high, mid, low


def product(a, b):
    def d(p, q):
        return jnp.dot(a[p], b[q], preferred_element_type=jnp.float32)
    return ((d(2, 0) + d(0, 2) + d(1, 1)) + (d(1, 0) + d(0, 1))) + d(0, 0)


def kernel(ts, v_ref, t_ref, z_ref, out_ref, vb_ref, tb_ref, xs, vv, ws, gs, yp, tv, stage, xr, ystage, yr,
           recv, recv_t, snd, snd_t, lsem, tsem, zsem, osem, xsend, xrecv, ysend, yrecv):
    hb = ts // 2
    us = 2 * ts
    z = lax.axis_index("row")
    col = lax.axis_index("col")
    core = lax.rem(col, 2)
    x = lax.rem(col // 2, 2)
    y = col // 4
    half = NU // 2

    def flip(q):
        nx = jnp.where(q == 0, 1 - x, x)
        ny = jnp.where(q == 1, 1 - y, y)
        nz = jnp.where(q == 2, 1 - z, z)
        return (nz, (ny * 2 + nx) * 2 + core)

    sibling = (z, col + 1 - 2 * core)

    zcopy = pltpu.make_async_copy(z_ref, xs, zsem)
    zcopy.start()
    barrier = pltpu.get_barrier_semaphore()
    for d in [flip(0), flip(1), flip(2), sibling]:
        pl.semaphore_signal(barrier, inc=1, device_id=d, device_id_type=MESH)
    pl.semaphore_wait(barrier, 4)

    def role(n, i, t):
        g = NCH - 1 - i
        ro = unit_of(i, t) // half
        co = g // 4
        ax = lax.rem(x + lax.rem(co // 2, 2), 2)
        ay = lax.rem(y + co // 4, 2)
        az = lax.rem(z + ro, 2)
        k = lax.rem(n, 3)
        a = jnp.where(k == 0, ax, jnp.where(k == 1, ay, az))
        b = jnp.where(k == 0, ay, jnp.where(k == 1, az, ax))
        c = jnp.where(k == 0, az, jnp.where(k == 1, ax, ay))
        s = a + b + c
        off = lax.rem(co + core, 2)
        depth = jnp.where(a == 1, s, jnp.where(s == 0, 0, 2 + s)) + off
        return k, a, b, c, s, off, depth

    def v_src(i, t, lane, size):
        g = NCH - 1 - i
        first = lax.rem(unit_of(i, t), half) * us + lane * ts
        return v_ref.at[pl.ds(pl.multiple_of(first, ts), size), pl.ds(pl.multiple_of(lax.rem(g, 4) * ts, ts), ts)]

    def short(i, t):
        return jnp.logical_and(t == 0, lax.rem(i, 2) == 0)

    def ship(root, n, i, t, lane, kind, to, dev):
        g = NCH - 1 - i
        there = vb_ref.at[n, pl.ds(pl.multiple_of(lane * ts, ts), ts)]
        t_there = tb_ref.at[i, lane]
        cv = pltpu.make_async_remote_copy(
            src_ref=v_src(i, t, lane, ts) if root else there, dst_ref=there,
            send_sem=snd.at[kind, lax.rem(n, RING)], recv_sem=recv.at[to, n], device_id=dev, device_id_type=MESH)
        ct = pltpu.make_async_remote_copy(
            src_ref=t_ref.at[lax.rem(g, 4) * 2 + lane] if root else t_there, dst_ref=t_there,
            send_sem=snd_t.at[kind, i], recv_sem=recv_t.at[to, i], device_id=dev, device_id_type=MESH)
        return cv, ct

    def both(i, t, lane, do_v, do_t):
        pl.when(jnp.logical_not(jnp.logical_and(short(i, t), lane == 0)))(do_v)
        pl.when(t == 0)(do_t)

    def start(root, n, i, t, lane, kind, to, dev):
        cv, ct = ship(root, n, i, t, lane, kind, to, dev)
        both(i, t, lane, cv.start, ct.start)

    def arrived(n, i, t, lane, to):
        cv, ct = ship(False, n, i, t, lane, 0, to, sibling)
        both(i, t, lane, cv.wait_recv, ct.wait_recv)

    def sent(n, i, t, lane, kind):
        cv, ct = ship(False, n, i, t, lane, kind, 0, sibling)
        both(i, t, lane, cv.wait_send, ct.wait_send)

    def slot(tau, st):
        st = list(st)
        for d in range(7):
            i, t = st[2 * d], st[2 * d + 1]
            n = tau - (d * HOP if d < 6 else LATE)
            live = jnp.logical_and(n >= 0, n < NT)
            k, a, b, c, s, off, depth = role(n, i, t)
            if d < 6:
                @pl.when(jnp.logical_and(live, depth == d))
                def _():
                    root = d == 0
                    if root:
                        start(root, n, i, t, core, 0, 0, flip(k))
                        start(root, n, i, t, 1 - core, 4, 0, sibling)
                        start(root, n, i, t, core, 3, 1, sibling)
                        return
                    arrived(n, i, t, core, 0)
                    if d < 5:
                        @pl.when(jnp.logical_or(s == 0, jnp.logical_and(a == 1, s >= 2)))
                        def _():
                            start(root, n, i, t, core, 0, 0, flip(k))
                    if d < 3:
                        @pl.when(jnp.logical_and(a == 1, s == 1))
                        def _():
                            start(root, n, i, t, core, 1, 0, flip(lax.rem(k + 1, 3)))
                    if d < 4:
                        @pl.when(jnp.logical_and(a == 1, c == 0))
                        def _():
                            start(root, n, i, t, core, 2, 0, flip(lax.rem(k + 2, 3)))

                    @pl.when(s > 0)
                    def _():
                        start(root, n, i, t, core, 3, 1, sibling)
            else:
                @pl.when(live)
                def _():
                    owner = s + off == 0

                    @pl.when(jnp.logical_not(owner))
                    def _():
                        arrived(n, i, t, 1 - core, 1)

                    @pl.when(jnp.logical_or(s > 0, off == 0))
                    def _():
                        sent(n, i, t, core, 3)

                    @pl.when(owner)
                    def _():
                        sent(n, i, t, 1 - core, 4)

                    @pl.when(jnp.logical_or(s == 0, jnp.logical_and(a == 1, s >= 2)))
                    def _():
                        sent(n, i, t, core, 0)

                    @pl.when(jnp.logical_and(a == 1, s == 1))
                    def _():
                        sent(n, i, t, core, 1)

                    @pl.when(jnp.logical_and(a == 1, c == 0))
                    def _():
                        sent(n, i, t, core, 2)
            end = t + 1 > i // 2
            st[2 * d] = jnp.where(n >= 0, jnp.where(end, i + 1, i), i)
            st[2 * d + 1] = jnp.where(n >= 0, jnp.where(end, 0, t + 1), t)
        return tuple(st)

    def is_owner(i, t):
        g = NCH - 1 - i
        return jnp.logical_and(g // 4 == col, unit_of(i, t) // half == z)

    def first_of(i):
        a = i // 2
        return a * (a + 1) + lax.rem(i, 2) * (a + 1)

    def load_or_wait(i, t, go):
        n = first_of(i) + t
        u = unit_of(i, t)
        sem = lsem.at[lax.rem(n, LRING)]

        def piece(own, skip):
            src = v_src(i, t, skip // ts, us - skip) if own else vb_ref.at[n, pl.ds(skip, us - skip)]
            dst = vv.at[lax.rem(i, 2), pl.ds(pl.multiple_of(u * us + skip, ts), us - skip)]
            return pltpu.make_async_copy(src, dst, sem)

        if not go:
            pl.when(short(i, t))(lambda: piece(False, ts).wait())
            pl.when(jnp.logical_not(short(i, t)))(lambda: piece(False, 0).wait())
            return
        own = is_owner(i, t)
        for o in (True, False):
            for skip in (0, ts):
                here = own if o else jnp.logical_not(own)
                part = short(i, t) if skip else jnp.logical_not(short(i, t))

                @pl.when(jnp.logical_and(here, part))
                def _():
                    piece(o, skip).start()

    def load(i, t):
        load_or_wait(i, t, True)

    def loaded(i, t):
        load_or_wait(i, t, False)

    def load_t(i):
        g = NCH - 1 - i
        own = is_owner(i, 0)
        sem = tsem.at[lax.rem(i, 2)]

        @pl.when(own)
        def _():
            pltpu.make_async_copy(t_ref.at[pl.ds(lax.rem(g, 4) * 2, 2)], tv.at[lax.rem(i, 2)], sem).start()

        @pl.when(jnp.logical_not(own))
        def _():
            pltpu.make_async_copy(tb_ref.at[i], tv.at[lax.rem(i, 2)], sem).start()

    def loaded_t(i):
        pltpu.make_async_copy(tb_ref.at[i], tv.at[lax.rem(i, 2)], tsem.at[lax.rem(i, 2)]).wait()

    def rows(u):
        return pl.ds(pl.multiple_of(u * us, us), us)

    other = (1 - z, col)

    def cross(q):
        return pltpu.make_async_remote_copy(
            src_ref=stage.at[rows(q)], dst_ref=xr.at[rows(q)], send_sem=xsend.at[q], recv_sem=xrecv.at[q],
            device_id=other, device_id_type=MESH)

    def cross_y(j):
        return pltpu.make_async_remote_copy(
            src_ref=ystage.at[j], dst_ref=yr.at[j], send_sem=ysend.at[j], recv_sem=yrecv.at[j],
            device_id=other, device_id_type=MESH)

    zero = jnp.int32(0)
    st = (zero,) * 14
    yp[...] = jnp.zeros_like(yp)

    def clear(q, carry):
        for p in range(2):
            vv[p, rows(q), :] = jnp.zeros((us, ts), jnp.float32)
        return carry

    lax.fori_loop(0, NU, clear, 0)
    st = lax.fori_loop(0, LAG, slot, st)
    zcopy.wait()
    load(zero, zero)

    def chunk(i, st):
        top = (NCH - 1 - i) // 2
        count = i // 2 + 1
        now = lax.rem(i, 2)
        old = 1 - now
        base = first_of(i)
        leaving = i == FIRST
        load_t(i)

        def prepare(t, st):
            st = slot(base + t + LAG, st)

            @pl.when(t + PRE < count)
            def _():
                load(i, t + PRE)
            return st

        def update(u):
            y = [yp[p] for p in range(3)]
            xs[rows(u), :] = xs[rows(u), :] - product(split(vv[old, rows(u), :]), y)

        def gather(u):
            v = vv[now, rows(u), :]
            return dot_t(v, xs[rows(u), :]), dot_t(v[:, :ts // 2], v[:, ts // 2:])

        def leave(u):
            @pl.when(jnp.logical_and(leaving, u // half == 1 - z))
            def _():
                stage[rows(lax.rem(u, half)), :] = xs[rows(u), :]

        def go(u):
            @pl.when(jnp.logical_and(leaving, u // half == 1 - z))
            def _():
                cross(lax.rem(u, half)).start()

        st = prepare(zero, st)
        update(top)
        leave(top)
        ws[...] = jnp.zeros_like(ws)
        gs[...] = jnp.zeros_like(gs)

        @pl.when(i == FIRST + 1)
        def _():
            cross_y(0).start()

        def unit(t, st):
            st = prepare(t, st)
            loaded(i, t - 1)
            u, v = unit_of(i, t - 1), unit_of(i, t)
            w, gg = gather(u)
            update(v)
            ws[...] += w
            gs[...] += gg
            leave(v)
            go(u)
            return st

        st = lax.fori_loop(1, count, unit, st)
        loaded(i, count - 1)
        w, gg = gather(unit_of(i, count - 1))
        ws[...] += w
        gs[...] += gg
        go(unit_of(i, count - 1))
        for p in range(PRE):
            @pl.when(jnp.logical_and(i + 1 < NCH, p < (i + 1) // 2 + 1))
            def _():
                load(i + 1, jnp.int32(p))
        loaded_t(i)
        y2 = dot(tv[now, 1], ws[hb:, :])
        y1 = dot(tv[now, 0], ws[:hb, :] - dot(gs[...], y2))
        for p, q in enumerate(split(y1)):
            yp[p, :hb, :] = q
        for p, q in enumerate(split(y2)):
            yp[p, hb:, :] = q

        @pl.when(i >= FIRST)
        def _():
            ystage[i - FIRST, :hb, :] = y1
            ystage[i - FIRST, hb:, :] = y2
        return st

    lax.fori_loop(0, NCH, chunk, st)

    def place(src, q, row, sem):
        return pltpu.make_async_copy(
            src, out_ref.at[rows(q), pl.ds(pl.multiple_of(row * ts, ts), ts)], sem)

    def mine(q):
        return place(xs.at[rows(half * z + q)], q, z, osem.at[q])

    def theirs(q):
        return place(xr.at[rows(q)], q, 1 - z, osem.at[half + q])

    def last(q, carry):
        y = [yp[p] for p in range(3)]
        r = rows(half * z + q)
        xs[r, :] = xs[r, :] - product(split(vv[(NCH - 1) % 2, r, :]), y)

        @pl.when(q == 0)
        def _():
            cross_y(1).start()

        @pl.when(q > 0)
        def _():
            mine(q - 1).start()
        return carry

    lax.fori_loop(0, half, last, 0)

    for j in range(2):
        cross_y(j).wait_recv()

    def last_theirs(q, carry):
        r = rows(half * z + q)
        cross(q).wait_recv()
        before = xr[rows(q), :] - dot(vv[FIRST % 2, r, :], yr[0])
        xr[rows(q), :] = before - dot(vv[1 - FIRST % 2, r, :], yr[1])

        @pl.when(q == 0)
        def _():
            mine(half - 1).start()

        @pl.when(q > 0)
        def _():
            theirs(q - 1).start()
        return carry

    lax.fori_loop(0, half, last_theirs, 0)
    for j in range(2):
        cross_y(j).wait_send()

    def drain(q, carry):
        mine(q).wait()
        cross(q).wait_send()
        return carry

    lax.fori_loop(0, half, drain, 0)
    theirs(half - 1).start()

    def drain_theirs(q, carry):
        theirs(q).wait()
        return carry

    lax.fori_loop(0, half, drain_theirs, 0)


def solution(mesh):
    def local_program(v_local, t_local, z_local):
        n = z_local.shape[0]
        ts = n // NCH
        f32 = jnp.float32
        any_ = pl.BlockSpec(memory_space=pl.ANY)
        dma = pltpu.SemaphoreType.DMA
        out, _, _ = pl.pallas_call(
            functools.partial(kernel, ts),
            out_shape=(jax.ShapeDtypeStruct((n // 2, 2 * ts), f32),
                       jax.ShapeDtypeStruct((NT, 2 * ts, ts), f32),
                       jax.ShapeDtypeStruct((NCH, 2, ts // 2, ts // 2), f32)),
            in_specs=[any_] * 3,
            out_specs=(any_,) * 3,
            scratch_shapes=[
                pltpu.VMEM((n, ts), f32),
                pltpu.VMEM((2, n, ts), f32),
                pltpu.VMEM((ts, ts), f32),
                pltpu.VMEM((ts // 2, ts // 2), f32),
                pltpu.VMEM((3, ts, ts), jnp.bfloat16),
                pltpu.VMEM((2, 2, ts // 2, ts // 2), f32),
                pltpu.VMEM((n // 2, ts), f32),
                pltpu.VMEM((n // 2, ts), f32),
                pltpu.VMEM((2, ts, ts), f32),
                pltpu.VMEM((2, ts, ts), f32),
                dma((2, NT)), dma((2, NCH)), dma((5, RING)), dma((5, NCH)),
                dma((LRING,)), dma((2,)), dma, dma((NU,)),
                dma((NU // 2,)), dma((NU // 2,)), dma((2,)), dma((2,)),
            ],
            compiler_params=pltpu.CompilerParams(collective_id=0, has_side_effects=True, vmem_limit_bytes=60 * 1024 * 1024),
            name="back_transform",
        )(v_local, t_local, z_local)
        return out

    return jax.shard_map(local_program, mesh=mesh, in_specs=(P("row", "col"), P("col", None, None), P(None, ("col", "row"))),
                         out_specs=P("row", "col"), check_vma=False)
```

```python
import functools

import jax
import jax.numpy as jnp
from jax import lax
from jax.experimental import pallas as pl
from jax.experimental.pallas import tpu as pltpu
from jax.sharding import PartitionSpec as P

HI = lax.Precision.HIGHEST
MESH = pl.DeviceIdType.MESH
NCH = 32
NU = NCH // 2
NT = NU * (NU + 1)
HOP = 6
PRE = 2
LATE = 5 * HOP + 2
LAG = LATE + PRE
RING = 64
LRING = 4
EARLY = 5
FIRST = NCH - 2


def dot(a, b):
    return jnp.dot(a, b, precision=HI, preferred_element_type=jnp.float32)


def dot_t(a, b):
    return lax.dot_general(a, b, (((0,), (0,)), ((), ())), precision=HI, preferred_element_type=jnp.float32)


def unit_of(i, t):
    half = NU // 2
    top = (NCH - 1 - i) // 2
    inner = jnp.where(lax.rem(t, 2) == 0, top + t // 2, half + t // 2)
    return jnp.where(t < 2 * (half - top), inner, top + t)


def split(v):
    high = v.astype(jnp.bfloat16)
    rest = v - high.astype(jnp.float32)
    mid = rest.astype(jnp.bfloat16)
    low = (rest - mid.astype(jnp.float32)).astype(jnp.bfloat16)
    return high, mid, low


def product(a, b):
    def d(p, q):
        return jnp.dot(a[p], b[q], preferred_element_type=jnp.float32)
    return ((d(2, 0) + d(0, 2) + d(1, 1)) + (d(1, 0) + d(0, 1))) + d(0, 0)


def kernel(ts, v_ref, t_ref, z_ref, out_ref, vb_ref, tb_ref, xs, vv, ws, gs, yp, tv, stage, xr, ystage, yr,
           recv, recv_t, snd, snd_t, lsem, tsem, zsem, osem, xsend, xrecv, ysend, yrecv):
    hb = ts // 2
    us = 2 * ts
    z = lax.axis_index("row")
    col = lax.axis_index("col")
    core = lax.rem(col, 2)
    x = lax.rem(col // 2, 2)
    y = col // 4
    half = NU // 2

    def flip(q):
        nx = jnp.where(q == 0, 1 - x, x)
        ny = jnp.where(q == 1, 1 - y, y)
        nz = jnp.where(q == 2, 1 - z, z)
        return (nz, (ny * 2 + nx) * 2 + core)

    sibling = (z, col + 1 - 2 * core)

    zcopy = pltpu.make_async_copy(z_ref, xs, zsem)
    zcopy.start()
    barrier = pltpu.get_barrier_semaphore()
    for d in [flip(0), flip(1), flip(2), sibling]:
        pl.semaphore_signal(barrier, inc=1, device_id=d, device_id_type=MESH)
    pl.semaphore_wait(barrier, 4)

    def role(n, i, t):
        g = NCH - 1 - i
        ro = unit_of(i, t) // half
        co = g // 4
        ax = lax.rem(x + lax.rem(co // 2, 2), 2)
        ay = lax.rem(y + co // 4, 2)
        az = lax.rem(z + ro, 2)
        k = lax.rem(n, 3)
        a = jnp.where(k == 0, ax, jnp.where(k == 1, ay, az))
        b = jnp.where(k == 0, ay, jnp.where(k == 1, az, ax))
        c = jnp.where(k == 0, az, jnp.where(k == 1, ax, ay))
        s = a + b + c
        off = lax.rem(co + core, 2)
        depth = jnp.where(a == 1, s, jnp.where(s == 0, 0, 2 + s)) + off
        return k, a, b, c, s, off, depth

    def v_src(i, t, lane, size):
        g = NCH - 1 - i
        first = lax.rem(unit_of(i, t), half) * us + lane * ts
        return v_ref.at[pl.ds(pl.multiple_of(first, ts), size), pl.ds(pl.multiple_of(lax.rem(g, 4) * ts, ts), ts)]

    def short(i, t):
        return jnp.logical_and(t == 0, lax.rem(i, 2) == 0)

    def ship(root, n, i, t, lane, kind, to, dev):
        g = NCH - 1 - i
        there = vb_ref.at[n, pl.ds(pl.multiple_of(lane * ts, ts), ts)]
        t_there = tb_ref.at[i, lane]
        cv = pltpu.make_async_remote_copy(
            src_ref=v_src(i, t, lane, ts) if root else there, dst_ref=there,
            send_sem=snd.at[kind, lax.rem(n, RING)], recv_sem=recv.at[to, n], device_id=dev, device_id_type=MESH)
        ct = pltpu.make_async_remote_copy(
            src_ref=t_ref.at[lax.rem(g, 4) * 2 + lane] if root else t_there, dst_ref=t_there,
            send_sem=snd_t.at[kind, i], recv_sem=recv_t.at[to, i], device_id=dev, device_id_type=MESH)
        return cv, ct

    def both(i, t, lane, do_v, do_t):
        pl.when(jnp.logical_not(jnp.logical_and(short(i, t), lane == 0)))(do_v)
        pl.when(t == 0)(do_t)

    def start(root, n, i, t, lane, kind, to, dev):
        cv, ct = ship(root, n, i, t, lane, kind, to, dev)
        both(i, t, lane, cv.start, ct.start)

    def arrived(n, i, t, lane, to):
        cv, ct = ship(False, n, i, t, lane, 0, to, sibling)
        both(i, t, lane, cv.wait_recv, ct.wait_recv)

    def sent(n, i, t, lane, kind):
        cv, ct = ship(False, n, i, t, lane, kind, 0, sibling)
        both(i, t, lane, cv.wait_send, ct.wait_send)

    def slot(tau, st):
        st = list(st)
        for d in range(7):
            i, t = st[2 * d], st[2 * d + 1]
            n = tau - (d * HOP if d < 6 else LATE)
            live = jnp.logical_and(n >= 0, n < NT)
            k, a, b, c, s, off, depth = role(n, i, t)
            if d < 6:
                @pl.when(jnp.logical_and(live, depth == d))
                def _():
                    root = d == 0
                    if root:
                        start(root, n, i, t, core, 0, 0, flip(k))
                        start(root, n, i, t, 1 - core, 4, 0, sibling)
                        start(root, n, i, t, core, 3, 1, sibling)
                        return
                    arrived(n, i, t, core, 0)
                    if d < 5:
                        @pl.when(jnp.logical_or(s == 0, jnp.logical_and(a == 1, s >= 2)))
                        def _():
                            start(root, n, i, t, core, 0, 0, flip(k))
                    if d < 3:
                        @pl.when(jnp.logical_and(a == 1, s == 1))
                        def _():
                            start(root, n, i, t, core, 1, 0, flip(lax.rem(k + 1, 3)))
                    if d < 4:
                        @pl.when(jnp.logical_and(a == 1, c == 0))
                        def _():
                            start(root, n, i, t, core, 2, 0, flip(lax.rem(k + 2, 3)))

                    @pl.when(s > 0)
                    def _():
                        start(root, n, i, t, core, 3, 1, sibling)
            else:
                @pl.when(live)
                def _():
                    owner = s + off == 0

                    @pl.when(jnp.logical_not(owner))
                    def _():
                        arrived(n, i, t, 1 - core, 1)

                    @pl.when(jnp.logical_or(s > 0, off == 0))
                    def _():
                        sent(n, i, t, core, 3)

                    @pl.when(owner)
                    def _():
                        sent(n, i, t, 1 - core, 4)

                    @pl.when(jnp.logical_or(s == 0, jnp.logical_and(a == 1, s >= 2)))
                    def _():
                        sent(n, i, t, core, 0)

                    @pl.when(jnp.logical_and(a == 1, s == 1))
                    def _():
                        sent(n, i, t, core, 1)

                    @pl.when(jnp.logical_and(a == 1, c == 0))
                    def _():
                        sent(n, i, t, core, 2)
            end = t + 1 > i // 2
            st[2 * d] = jnp.where(n >= 0, jnp.where(end, i + 1, i), i)
            st[2 * d + 1] = jnp.where(n >= 0, jnp.where(end, 0, t + 1), t)
        return tuple(st)

    def is_owner(i, t):
        g = NCH - 1 - i
        return jnp.logical_and(g // 4 == col, unit_of(i, t) // half == z)

    def first_of(i):
        a = i // 2
        return a * (a + 1) + lax.rem(i, 2) * (a + 1)

    def load_or_wait(i, t, go):
        n = first_of(i) + t
        u = unit_of(i, t)
        sem = lsem.at[lax.rem(n, LRING)]

        def piece(own, skip):
            src = v_src(i, t, skip // ts, us - skip) if own else vb_ref.at[n, pl.ds(skip, us - skip)]
            dst = vv.at[lax.rem(i, 2), pl.ds(pl.multiple_of(u * us + skip, ts), us - skip)]
            return pltpu.make_async_copy(src, dst, sem)

        if not go:
            pl.when(short(i, t))(lambda: piece(False, ts).wait())
            pl.when(jnp.logical_not(short(i, t)))(lambda: piece(False, 0).wait())
            return
        own = is_owner(i, t)
        for o in (True, False):
            for skip in (0, ts):
                here = own if o else jnp.logical_not(own)
                part = short(i, t) if skip else jnp.logical_not(short(i, t))

                @pl.when(jnp.logical_and(here, part))
                def _():
                    piece(o, skip).start()

    def load(i, t):
        load_or_wait(i, t, True)

    def loaded(i, t):
        load_or_wait(i, t, False)

    def load_t(i):
        g = NCH - 1 - i
        own = is_owner(i, 0)
        sem = tsem.at[lax.rem(i, 2)]

        @pl.when(own)
        def _():
            pltpu.make_async_copy(t_ref.at[pl.ds(lax.rem(g, 4) * 2, 2)], tv.at[lax.rem(i, 2)], sem).start()

        @pl.when(jnp.logical_not(own))
        def _():
            pltpu.make_async_copy(tb_ref.at[i], tv.at[lax.rem(i, 2)], sem).start()

    def loaded_t(i):
        pltpu.make_async_copy(tb_ref.at[i], tv.at[lax.rem(i, 2)], tsem.at[lax.rem(i, 2)]).wait()

    def rows(u):
        return pl.ds(pl.multiple_of(u * us, us), us)

    other = (1 - z, col)

    def cross(q):
        return pltpu.make_async_remote_copy(
            src_ref=stage.at[rows(q)], dst_ref=xr.at[rows(q)], send_sem=xsend.at[q], recv_sem=xrecv.at[q],
            device_id=other, device_id_type=MESH)

    def cross_y(j):
        return pltpu.make_async_remote_copy(
            src_ref=ystage.at[j], dst_ref=yr.at[j], send_sem=ysend.at[j], recv_sem=yrecv.at[j],
            device_id=other, device_id_type=MESH)

    zero = jnp.int32(0)
    st = (zero,) * 14
    yp[...] = jnp.zeros_like(yp)

    def clear(q, carry):
        for p in range(2):
            vv[p, rows(q), :] = jnp.zeros((us, ts), jnp.float32)
        return carry

    lax.fori_loop(0, NU, clear, 0)
    st = lax.fori_loop(0, LAG, slot, st)
    zcopy.wait()
    load(zero, zero)

    def chunk(i, st):
        top = (NCH - 1 - i) // 2
        count = i // 2 + 1
        now = lax.rem(i, 2)
        old = 1 - now
        base = first_of(i)
        leaving = i == FIRST
        load_t(i)

        def prepare(t, st):
            st = slot(base + t + LAG, st)

            @pl.when(t + PRE < count)
            def _():
                load(i, t + PRE)
            return st

        def update(u):
            y = [yp[p] for p in range(3)]
            xs[rows(u), :] = xs[rows(u), :] - product(split(vv[old, rows(u), :]), y)

        def gather(u):
            v = vv[now, rows(u), :]
            return dot_t(v, xs[rows(u), :]), dot_t(v[:, :ts // 2], v[:, ts // 2:])

        def leave(u):
            @pl.when(jnp.logical_and(leaving, u // half == 1 - z))
            def _():
                stage[rows(lax.rem(u, half)), :] = xs[rows(u), :]

        def go(u):
            q = lax.rem(u, half)

            @pl.when(jnp.logical_and(leaving, jnp.logical_and(u // half == 1 - z, q < EARLY)))
            def _():
                cross(q).start()

        st = prepare(zero, st)
        update(top)
        leave(top)
        ws[...] = jnp.zeros_like(ws)
        gs[...] = jnp.zeros_like(gs)

        @pl.when(i == FIRST + 1)
        def _():
            cross_y(0).start()

        def unit(t, st):
            st = prepare(t, st)
            loaded(i, t - 1)
            u, v = unit_of(i, t - 1), unit_of(i, t)
            w, gg = gather(u)
            update(v)
            ws[...] += w
            gs[...] += gg
            leave(v)
            go(u)
            return st

        st = lax.fori_loop(1, count, unit, st)
        loaded(i, count - 1)
        w, gg = gather(unit_of(i, count - 1))
        ws[...] += w
        gs[...] += gg
        go(unit_of(i, count - 1))
        for p in range(PRE):
            @pl.when(jnp.logical_and(i + 1 < NCH, p < (i + 1) // 2 + 1))
            def _():
                load(i + 1, jnp.int32(p))
        loaded_t(i)
        y2 = dot(tv[now, 1], ws[hb:, :])
        y1 = dot(tv[now, 0], ws[:hb, :] - dot(gs[...], y2))
        for p, q in enumerate(split(y1)):
            yp[p, :hb, :] = q
        for p, q in enumerate(split(y2)):
            yp[p, hb:, :] = q

        @pl.when(i >= FIRST)
        def _():
            ystage[i - FIRST, :hb, :] = y1
            ystage[i - FIRST, hb:, :] = y2
        return st

    lax.fori_loop(0, NCH, chunk, st)

    def place(src, q, row, sem):
        return pltpu.make_async_copy(
            src, out_ref.at[rows(q), pl.ds(pl.multiple_of(row * ts, ts), ts)], sem)

    def mine(q):
        return place(xs.at[rows(half * z + q)], q, z, osem.at[q])

    def theirs(q):
        return place(xr.at[rows(q)], q, 1 - z, osem.at[half + q])

    def last(q, carry):
        y = [yp[p] for p in range(3)]
        r = rows(half * z + q)
        xs[r, :] = xs[r, :] - product(split(vv[(NCH - 1) % 2, r, :]), y)

        @pl.when(q == 0)
        def _():
            cross_y(1).start()
            for p in range(EARLY, half):
                cross(p).start()

        @pl.when(q > 0)
        def _():
            mine(q - 1).start()
        return carry

    lax.fori_loop(0, half, last, 0)

    for j in range(2):
        cross_y(j).wait_recv()

    def last_theirs(q, carry):
        r = rows(half * z + q)
        cross(q).wait_recv()
        before = xr[rows(q), :] - dot(vv[FIRST % 2, r, :], yr[0])
        xr[rows(q), :] = before - dot(vv[1 - FIRST % 2, r, :], yr[1])

        @pl.when(q == 0)
        def _():
            mine(half - 1).start()

        @pl.when(q > 0)
        def _():
            theirs(q - 1).start()
        return carry

    lax.fori_loop(0, half, last_theirs, 0)
    for j in range(2):
        cross_y(j).wait_send()

    def drain(q, carry):
        mine(q).wait()
        cross(q).wait_send()
        return carry

    lax.fori_loop(0, half, drain, 0)
    theirs(half - 1).start()

    def drain_theirs(q, carry):
        theirs(q).wait()
        return carry

    lax.fori_loop(0, half, drain_theirs, 0)


def solution(mesh):
    def local_program(v_local, t_local, z_local):
        n = z_local.shape[0]
        ts = n // NCH
        f32 = jnp.float32
        any_ = pl.BlockSpec(memory_space=pl.ANY)
        dma = pltpu.SemaphoreType.DMA
        out, _, _ = pl.pallas_call(
            functools.partial(kernel, ts),
            out_shape=(jax.ShapeDtypeStruct((n // 2, 2 * ts), f32),
                       jax.ShapeDtypeStruct((NT, 2 * ts, ts), f32),
                       jax.ShapeDtypeStruct((NCH, 2, ts // 2, ts // 2), f32)),
            in_specs=[any_] * 3,
            out_specs=(any_,) * 3,
            scratch_shapes=[
                pltpu.VMEM((n, ts), f32),
                pltpu.VMEM((2, n, ts), f32),
                pltpu.VMEM((ts, ts), f32),
                pltpu.VMEM((ts // 2, ts // 2), f32),
                pltpu.VMEM((3, ts, ts), jnp.bfloat16),
                pltpu.VMEM((2, 2, ts // 2, ts // 2), f32),
                pltpu.VMEM((n // 2, ts), f32),
                pltpu.VMEM((n // 2, ts), f32),
                pltpu.VMEM((2, ts, ts), f32),
                pltpu.VMEM((2, ts, ts), f32),
                dma((2, NT)), dma((2, NCH)), dma((5, RING)), dma((5, NCH)),
                dma((LRING,)), dma((2,)), dma, dma((NU,)),
                dma((NU // 2,)), dma((NU // 2,)), dma((2,)), dma((2,)),
            ],
            compiler_params=pltpu.CompilerParams(collective_id=0, has_side_effects=True, vmem_limit_bytes=60 * 1024 * 1024),
            name="back_transform",
        )(v_local, t_local, z_local)
        return out

    return jax.shard_map(local_program, mesh=mesh, in_specs=(P("row", "col"), P("col", None, None), P(None, ("col", "row"))),
                         out_specs=P("row", "col"), check_vma=False)
```
